32 devices in a mesh: dp: 8 (over y, x, core), mp: 4 (over z).
Axes of the slice: x: 2, y: 2, z: 4, core: 2. Of those that a mesh axis runs over, the one named last changes fastest.
Arguments:
- images: bfloat16 [1536, 1024], P('dp', 'mp'), may hold values from -80 to 80, as said below
- texts: bfloat16 [1536, 1024], P('dp', 'mp'), may hold values from -80 to 80, as said below
- logit_scale: float32 [1], replicated, may hold values from 240 to 300
Outputs:
- row_loss: float32 [1536], P('dp')
- column_loss: float32 [1536], P('dp')
The draws below stay inside these ranges and needn't reach their ends.
Inputs may be any that keep to these rules, and one draw needn't show every extreme that they name: `images`: Real-valued entries. `texts`: Real-valued entries.
All inputs are finite; a program needn't handle non-finite values.
Results may differ from the reference program's by a relative error of at most 0.0044.
Values may be sent and summed in bfloat16 or wider, within the bound.
No kernel may reach another device: no remote copies, remote signals or barrier semaphores. Data moves between devices by JAX's collectives and lax.ppermute only.
A program may use at most 64 MiB of HBM per device.

```python
import jax
import jax.numpy as jnp
from jax import lax

D = 1024
ROWS_DEV = 192
BATCH = 1536
N_DP = 8


def draw_pair(key):
    image_key = jax.random.fold_in(key, 11)
    text_key = jax.random.fold_in(key, 12)
    common_key = jax.random.fold_in(key, 15)
    spread_key = jax.random.fold_in(key, 16)
    common = jax.random.normal(common_key, (1, D), jnp.float32)
    block_spread = jnp.exp(jax.random.uniform(spread_key, (BATCH // ROWS_DEV,), jnp.float32, jnp.log(0.03), 0.0))
    spread = block_spread[jnp.arange(BATCH) // ROWS_DEV][:, None]
    weight = jnp.sqrt(1.0 - spread * spread)
    image_rows = weight * common + spread * jax.random.normal(image_key, (BATCH, D), jnp.float32)
    text_rows = jax.random.normal(text_key, (BATCH, D), jnp.float32)
    image_rows = jnp.clip(image_rows, -80.0, 80.0)
    text_rows = jnp.clip(text_rows, -80.0, 80.0)
    return (image_rows, text_rows)


def draw_images(key, part):
    return draw_pair(key)[0].astype(jnp.bfloat16)


def draw_texts(key, part):
    return draw_pair(key)[1].astype(jnp.bfloat16)


def setup_inputs(seed: int = 0) -> dict:
    streams_of = jax.random.split(jax.random.key(seed), 4)
    return {
        "images": draw_images(jax.random.fold_in(streams_of[3], 71), 0),
        "texts": draw_texts(jax.random.fold_in(streams_of[3], 71), 0),
        "logit_scale": jnp.clip(jax.random.uniform(streams_of[2], (1,), jnp.float32, 240.0, 300.0), 240.0, 300.0),
    }


def normalize(rows):
    values = rows.astype(jnp.float32)
    return (values * lax.rsqrt(lax.optimization_barrier(jnp.sum(values * values, axis=1, keepdims=True)) + 1e-06)).astype(jnp.bfloat16)

def reference(images, texts, logit_scale):
    image_unit = normalize(images)
    text_unit = normalize(texts)
    inverse_temp = logit_scale[0]
    matched = inverse_temp * lax.optimization_barrier(jnp.sum(image_unit.astype(jnp.float32) * text_unit.astype(jnp.float32), axis=1))
    blocks = text_unit.reshape(N_DP, ROWS_DEV, D)

    def visit(states, block):
        row_top, row_total = states
        scores = inverse_temp * jnp.dot(block, image_unit.T, preferred_element_type=jnp.float32)
        column_top = lax.optimization_barrier(jnp.max(scores, axis=1))
        column_lse = column_top + jnp.log(lax.optimization_barrier(jnp.sum(jnp.exp(scores - column_top[:, None]), axis=1)))
        new_top = jnp.maximum(row_top, lax.optimization_barrier(jnp.max(scores, axis=0)))
        row_total = row_total * jnp.exp(row_top - new_top) + lax.optimization_barrier(jnp.sum(jnp.exp(scores - new_top[None, :]), axis=0))
        return ((new_top, row_total), column_lse)
    start = (jnp.full((BATCH,), -1e+30, jnp.float32), jnp.zeros((BATCH,), jnp.float32))
    (row_top, row_total), column_lse = lax.scan(visit, start, blocks)
    row_loss = row_top + jnp.log(row_total) - matched
    column_loss = column_lse.reshape(-1) - matched
    return (row_loss, column_loss)
```

```python
import jax
import jax.numpy as jnp
from jax import lax
from jax.sharding import PartitionSpec as P

AXES = ("dp", "mp")


def normalize(rows):
    values = rows.astype(jnp.float32)
    return (values * lax.rsqrt(jnp.sum(values * values, axis=1, keepdims=True) + 1e-06)).astype(
        jnp.bfloat16
    )


def shift(x, axis, step):
    return lax.ppermute(x, axis, [(i, i ^ step) for i in range(lax.axis_size(axis))])


def on_device(images, texts, logit_scale):
    n = lax.axis_size("dp")
    q = lax.axis_size("mp")
    i = lax.axis_index("dp")
    k = lax.axis_index("mp")
    scale = logit_scale[0]
    rows, width = images.shape
    quarter = rows // q
    parts = texts.reshape(q, quarter, width)
    text_parts = [lax.dynamic_index_in_dim(parts, k, 0, False)]
    for s in range(1, q):
        text_parts.append(shift(lax.dynamic_index_in_dim(parts, k ^ s, 0, False), "mp", s))
    image_parts = [images] + [shift(images, "mp", s) for s in range(1, q)]
    text_unit = normalize(jnp.concatenate(text_parts, axis=1))
    if n == 8:
        got = {0: text_unit}
        for d in range(2, n, 2):
            got[d] = shift(text_unit, "dp", d)
        for d in range(0, n, 2):
            got[d + 1] = shift(got[d], "dp", 1)
        all_texts = jnp.concatenate([got[d] for d in range(n)], axis=0)
        order = i ^ jnp.arange(n)
    else:
        all_texts = lax.all_gather(text_unit, "dp", axis=0, tiled=True)
        order = jnp.arange(n)
    image_unit = normalize(jnp.concatenate(image_parts, axis=1))
    scores = scale * lax.dot_general(
        image_unit, all_texts, (((1,), (1,)), ((), ())), preferred_element_type=jnp.float32
    )
    row_top = jnp.max(scores, axis=1)
    row_lse = row_top + jnp.log(jnp.sum(jnp.exp(scores - row_top[:, None]), axis=1))
    col_top = jnp.max(scores, axis=0)
    col_lse = col_top + jnp.log(jnp.sum(jnp.exp(scores - col_top[None, :]), axis=0))
    mine = lax.dynamic_slice_in_dim(image_unit, k * quarter, quarter, 0)
    matched = scale * jnp.sum(mine.astype(jnp.float32) * text_unit.astype(jnp.float32), axis=1)
    col_lse = col_lse.reshape(n, quarter)[order]
    pieces = [
        jnp.broadcast_to(row_lse[None], (n, rows)),
        jnp.broadcast_to(matched[None], (n, quarter)),
        col_lse,
    ]
    message = jnp.concatenate(pieces, axis=1)
    size = message.shape[1]
    lanes = -(-size // 128) * 128
    message = jnp.pad(message, ((0, 0), (0, lanes - size)))
    message = jnp.broadcast_to(message[:, None, :], (n, q, lanes)).reshape(n * q, lanes // 128, 128)
    got = lax.all_to_all(message, AXES, 0, 0, tiled=True).reshape(n, q, lanes)
    own = lax.dynamic_index_in_dim(got, i, 0, False)
    row_parts = own[:, :rows]
    peak = jnp.max(row_parts, axis=0)
    row_out = peak + jnp.log(jnp.sum(jnp.exp(row_parts - peak), axis=0))
    matched = own[:, rows : rows + quarter].reshape(rows)
    col_parts = got[:, :, rows + quarter : size]
    peak = jnp.max(col_parts, axis=0)
    col_out = (peak + jnp.log(jnp.sum(jnp.exp(col_parts - peak), axis=0))).reshape(rows)
    return row_out - matched, col_out - matched


def solution(mesh):
    return jax.shard_map(
        on_device,
        mesh=mesh,
        in_specs=(P("dp", "mp"), P("dp", "mp"), P()),
        out_specs=(P("dp"), P("dp")),
        check_vma=False,
    )
```

```python
import functools

import jax
import jax.numpy as jnp
from jax import lax
from jax.experimental import pallas as pl
from jax.experimental.pallas import tpu as pltpu
from jax.sharding import PartitionSpec as P

AXES = ("dp", "mp")
LANES = 128
F32 = jnp.float32
BF16 = jnp.bfloat16


def normalize(rows):
    values = rows.astype(F32)
    return (values * lax.rsqrt(jnp.sum(values * values, axis=1, keepdims=True) + 1e-06)).astype(
        BF16
    )


def shift(x, axis, step):
    return lax.ppermute(x, axis, [(i, i ^ step) for i in range(lax.axis_size(axis))])


def local_kernel(body, out_shape, operands, out_memory=pltpu.VMEM):
    outs = jax.tree.leaves(out_shape)
    return pl.pallas_call(
        body,
        out_shape=out_shape,
        in_specs=[pl.BlockSpec(memory_space=pltpu.VMEM)] * len(operands),
        out_specs=jax.tree.map(lambda _: pl.BlockSpec(memory_space=out_memory), out_shape),
        compiler_params=pltpu.CompilerParams(vmem_limit_bytes=8 * 2**20),
    )(*operands)


def split_body(quarter, texts_ref, *out_refs):
    k = lax.axis_index("mp")
    for s, out_ref in enumerate(out_refs):
        start = pl.multiple_of((k ^ s) * quarter, 8)
        out_ref[...] = texts_ref[pl.ds(start, quarter), :]


def unit_body(*refs):
    out_ref = refs[-1]
    parts = [ref[...].astype(F32) for ref in refs[:-1]]
    total = sum(jnp.sum(part * part, axis=1, keepdims=True) for part in parts)
    inverse = lax.rsqrt(total + 1e-06)
    width = parts[0].shape[1]
    for s, part in enumerate(parts):
        out_ref[:, s * width : (s + 1) * width] = (part * inverse).astype(BF16)


def to_lanes(column, first):
    count = column.shape[0]
    row = lax.broadcasted_iota(jnp.int32, (count, LANES), 0)
    lane = lax.broadcasted_iota(jnp.int32, (count, LANES), 1)
    return jnp.sum(jnp.where(row + first == lane, column, 0.0), axis=0, keepdims=True)


def stats_body(n, q, scale_ref, image_ref, *refs):
    text_refs, out_ref = refs[:-1], refs[-1]
    i = lax.axis_index("dp")
    k = lax.axis_index("mp")
    image = image_ref[...]
    rows = image.shape[0]
    quarter = text_refs[0].shape[0]
    text = jnp.concatenate([ref[...] for ref in text_refs], axis=0)
    scores = scale_ref[0] * lax.dot_general(
        text, image, (((1,), (1,)), ((), ())), preferred_element_type=F32
    )
    row_top = jnp.max(scores, axis=0, keepdims=True)
    row_lse = row_top + jnp.log(jnp.sum(jnp.exp(scores - row_top), axis=0, keepdims=True))
    col_top = jnp.max(scores, axis=1, keepdims=True)
    col_lse = col_top + jnp.log(jnp.sum(jnp.exp(scores - col_top), axis=1, keepdims=True))
    own = scores[:quarter]
    row = lax.broadcasted_iota(jnp.int32, own.shape, 0)
    lane = lax.broadcasted_iota(jnp.int32, own.shape, 1)
    matched = jnp.sum(jnp.where(row + k * quarter == lane, own, 0.0), axis=1, keepdims=True)
    spare = jnp.zeros((1, 2 * LANES - rows), F32)
    wide = jnp.concatenate([row_lse, spare], axis=1)
    matched = to_lanes(matched, 0)
    for d in range(n):
        col = to_lanes(col_lse[d * quarter : (d + 1) * quarter], 0)
        block = jnp.concatenate([wide[:, :LANES], wide[:, LANES:], col, matched], axis=0)
        for m in range(q):
            out_ref[(i ^ d) * q + m] = block


def finish_body(n, q, rows, got_ref, row_ref, col_ref):
    i = lax.axis_index("dp")
    quarter = rows // q
    own = [got_ref[i * q + m] for m in range(q)]
    peak = functools.reduce(jnp.maximum, own)
    lse = peak + jnp.log(sum(jnp.exp(x - peak) for x in own))
    row_lse = jnp.concatenate([lse[0:1], lse[1:2]], axis=1)[:, :rows]
    matched = jnp.concatenate([x[3:4, :quarter] for x in own], axis=1)
    cols = []
    for m in range(q):
        parts = [got_ref[j * q + m] for j in range(n)]
        peak = functools.reduce(jnp.maximum, parts)
        lse = peak + jnp.log(sum(jnp.exp(x - peak) for x in parts))
        cols.append(lse[2:3, :quarter])
    row_ref[...] = (row_lse - matched).reshape(rows)
    col_ref[...] = (jnp.concatenate(cols, axis=1) - matched).reshape(rows)


def cube(images, texts, logit_scale):
    n = lax.axis_size("dp")
    q = lax.axis_size("mp")
    rows, width = images.shape
    quarter = rows // q
    part = jax.ShapeDtypeStruct((quarter, width), BF16)
    text_parts = local_kernel(functools.partial(split_body, quarter), [part] * q, [texts])
    got = [text_parts[0]]
    for s in range(1, q):
        with jax.named_scope(f"t{s}"):
            got.append(shift(text_parts[s], "mp", s))
    image_parts = [images]
    for s in range(1, q):
        with jax.named_scope(f"i{s}"):
            image_parts.append(shift(images, "mp", s))
    text_unit = local_kernel(unit_body, jax.ShapeDtypeStruct((quarter, q * width), BF16), got)
    blocks = {0: text_unit}
    for d in range(2, n, 2):
        with jax.named_scope(f"p{d}"):
            blocks[d] = shift(text_unit, "dp", d)
    for d in range(0, n, 2):
        with jax.named_scope(f"c{d}"):
            blocks[d + 1] = shift(blocks[d], "dp", 1)
    image_unit = local_kernel(
        unit_body, jax.ShapeDtypeStruct((rows, q * width), BF16), image_parts
    )
    message = pl.pallas_call(
        functools.partial(stats_body, n, q),
        out_shape=jax.ShapeDtypeStruct((n * q, 4, LANES), F32),
        in_specs=[pl.BlockSpec(memory_space=pltpu.SMEM)]
        + [pl.BlockSpec(memory_space=pltpu.VMEM)] * (n + 1),
        out_specs=pl.BlockSpec(memory_space=pltpu.VMEM),
        compiler_params=pltpu.CompilerParams(vmem_limit_bytes=8 * 2**20),
    )(logit_scale, image_unit, *[blocks[d] for d in range(n)])
    answer = lax.all_to_all(message, AXES, 0, 0, tiled=True)
    loss = jax.ShapeDtypeStruct((rows,), F32)
    row_loss, column_loss = local_kernel(
        functools.partial(finish_body, n, q, rows), [loss, loss], [answer]
    )
    return row_loss, column_loss


def gathered(images, texts, logit_scale):
    n = lax.axis_size("dp")
    q = lax.axis_size("mp")
    i = lax.axis_index("dp")
    k = lax.axis_index("mp")
    scale = logit_scale[0]
    rows = images.shape[0]
    quarter = rows // q
    image_unit = normalize(lax.all_gather(images, "mp", axis=1, tiled=True))
    text_unit = normalize(lax.all_to_all(texts, "mp", split_axis=0, concat_axis=1, tiled=True))
    all_texts = lax.all_gather(text_unit, "dp", axis=0, tiled=True)
    scores = scale * lax.dot_general(
        image_unit, all_texts, (((1,), (1,)), ((), ())), preferred_element_type=F32
    )
    row_top = jnp.max(scores, axis=1)
    row_lse = row_top + jnp.log(jnp.sum(jnp.exp(scores - row_top[:, None]), axis=1))
    col_top = jnp.max(scores, axis=0)
    col_lse = col_top + jnp.log(jnp.sum(jnp.exp(scores - col_top[None, :]), axis=0))
    mine = lax.dynamic_slice_in_dim(image_unit, k * quarter, quarter, 0)
    matched = scale * jnp.sum(mine.astype(F32) * text_unit.astype(F32), axis=1)
    pieces = [
        jnp.broadcast_to(row_lse[None], (n, rows)),
        jnp.broadcast_to(matched[None], (n, quarter)),
        col_lse.reshape(n, quarter),
    ]
    message = jnp.concatenate(pieces, axis=1)
    size = message.shape[1]
    lanes = -(-size // LANES) * LANES
    message = jnp.pad(message, ((0, 0), (0, lanes - size)))
    message = jnp.broadcast_to(message[:, None, :], (n, q, lanes)).reshape(n * q, -1, LANES)
    got = lax.all_to_all(message, AXES, 0, 0, tiled=True).reshape(n, q, lanes)
    own = lax.dynamic_index_in_dim(got, i, 0, False)
    row_parts = own[:, :rows]
    peak = jnp.max(row_parts, axis=0)
    row_out = peak + jnp.log(jnp.sum(jnp.exp(row_parts - peak), axis=0))
    matched = own[:, rows : rows + quarter].reshape(rows)
    col_parts = got[:, :, rows + quarter : size]
    peak = jnp.max(col_parts, axis=0)
    col_out = (peak + jnp.log(jnp.sum(jnp.exp(col_parts - peak), axis=0))).reshape(rows)
    return row_out - matched, col_out - matched


def on_device(images, texts, logit_scale):
    n = lax.axis_size("dp")
    q = lax.axis_size("mp")
    power = n & (n - 1) == 0 and q & (q - 1) == 0
    rows, width = images.shape
    fits = LANES < rows <= 2 * LANES and rows // q <= LANES and width % LANES == 0
    if power and n <= 8 and q <= 4 and fits and (rows // q) % 16 == 0:
        return cube(images, texts, logit_scale)
    return gathered(images, texts, logit_scale)


def solution(mesh):
    return jax.shard_map(
        on_device,
        mesh=mesh,
        in_specs=(P("dp", "mp"), P("dp", "mp"), P()),
        out_specs=(P("dp"), P("dp")),
        check_vma=False,
    )
```

```python
import functools

import jax
import jax.numpy as jnp
from jax import lax
from jax.experimental import pallas as pl
from jax.experimental.pallas import tpu as pltpu
from jax.sharding import PartitionSpec as P


AXES = ("dp", "mp")
LANES = 128
F32 = jnp.float32
BF16 = jnp.bfloat16


def normalize(rows):
    values = rows.astype(F32)
    return (values * lax.rsqrt(jnp.sum(values * values, axis=1, keepdims=True) + 1e-06)).astype(
        BF16
    )


def shift(x, axis, step):
    return lax.ppermute(x, axis, [(i, i ^ step) for i in range(lax.axis_size(axis))])


def local_kernel(body, out_shape, operands, out_memory=pltpu.VMEM):
    outs = jax.tree.leaves(out_shape)
    return pl.pallas_call(
        body,
        out_shape=out_shape,
        in_specs=[pl.BlockSpec(memory_space=pltpu.VMEM)] * len(operands),
        out_specs=jax.tree.map(lambda _: pl.BlockSpec(memory_space=out_memory), out_shape),
        compiler_params=pltpu.CompilerParams(vmem_limit_bytes=8 * 2**20),
    )(*operands)


def split_body(quarter, texts_ref, *refs):
    half = len(refs) // 2
    k = lax.axis_index("mp")
    copies = []
    for s, (out_ref, sem) in enumerate(zip(refs[:half], refs[half:])):
        start = pl.multiple_of((k ^ s) * quarter, 8)
        copies.append(pltpu.make_async_copy(texts_ref.at[pl.ds(start, quarter)], out_ref, sem))
    for copy in copies:
        copy.start()
    for copy in copies:
        copy.wait()


def unit_body(*refs):
    out_ref = refs[-1]
    parts = [ref[...].astype(F32) for ref in refs[:-1]]
    total = sum(jnp.sum(part * part, axis=1, keepdims=True) for part in parts)
    inverse = lax.rsqrt(total + 1e-06)
    width = parts[0].shape[1]
    for s, part in enumerate(parts):
        out_ref[:, s * width : (s + 1) * width] = (part * inverse).astype(BF16)


def to_lanes(column):
    shape = (column.shape[0], LANES)
    row = lax.broadcasted_iota(jnp.int32, shape, 0)
    lane = lax.broadcasted_iota(jnp.int32, shape, 1)
    return jnp.sum(jnp.where(row == lane, column, 0.0), axis=0, keepdims=True)


def stats_body(n, q, scale_ref, *refs):
    image_refs, text_refs, out_ref = refs[:2], refs[2:-1], refs[-1]
    i = lax.axis_index("dp")
    k = lax.axis_index("mp")
    rows = image_refs[0].shape[0]
    quarter = text_refs[0].shape[0]
    text = jnp.concatenate([ref[...] for ref in text_refs], axis=0)
    scores = [
        scale_ref[0]
        * lax.dot_general(
            text, ref[...], (((1,), (1,)), ((), ())), preferred_element_type=F32
        )
        for ref in image_refs
    ]
    row_lse = []
    for part in scores:
        top = jnp.max(part, axis=0, keepdims=True)
        row_lse.append(top + jnp.log(jnp.sum(jnp.exp(part - top), axis=0, keepdims=True)))
    top = jnp.max(jnp.maximum(*scores), axis=1, keepdims=True)
    total = jnp.exp(scores[0] - top) + jnp.exp(scores[1] - top)
    col_lse = top + jnp.log(jnp.sum(total, axis=1, keepdims=True))
    own = scores[0][:quarter]
    row = lax.broadcasted_iota(jnp.int32, own.shape, 0)
    lane = lax.broadcasted_iota(jnp.int32, own.shape, 1)
    matched = jnp.sum(jnp.where(row + k * quarter == lane, own, 0.0), axis=1, keepdims=True)
    matched = to_lanes(matched)
    spare = jnp.zeros((1, 2 * LANES - rows), F32)
    wide = [jnp.concatenate([lse, spare], axis=1) for lse in row_lse]
    for d in range(n):
        lse = wide[d % 2]
        col = to_lanes(col_lse[d // 2 * quarter : (d // 2 + 1) * quarter])
        block = jnp.concatenate([lse[:, :LANES], lse[:, LANES:], col, matched], axis=0)
        for m in range(q):
            out_ref[(i ^ d) * q + m] = block


def finish_body(n, q, rows, got_ref, row_ref, col_ref):
    i = lax.axis_index("dp")
    quarter = rows // q

    def merge(parts):
        peak = functools.reduce(jnp.maximum, parts)
        return peak + jnp.log(sum(jnp.exp(x - peak) for x in parts))

    lse = merge([got_ref[(i ^ d) * q + m] for d in range(2) for m in range(q)])
    row_lse = jnp.concatenate([lse[0:1], lse[1:2]], axis=1)[:, :rows]
    own = [got_ref[i * q + m] for m in range(q)]
    matched = jnp.concatenate([x[3:4, :quarter] for x in own], axis=1)
    cols = []
    for m in range(q):
        lse = merge([got_ref[(i ^ d) * q + m] for d in range(0, n, 2)])
        cols.append(lse[2:3, :quarter])
    row_ref[...] = (row_lse - matched).reshape(rows)
    col_ref[...] = (jnp.concatenate(cols, axis=1) - matched).reshape(rows)


def cube(images, texts, logit_scale):
    n = lax.axis_size("dp")
    q = lax.axis_size("mp")
    rows, width = images.shape
    quarter = rows // q
    part = jax.ShapeDtypeStruct((quarter, width), BF16)
    text_parts = pl.pallas_call(
        functools.partial(split_body, quarter),
        out_shape=[part] * q,
        in_specs=[pl.BlockSpec(memory_space=pl.ANY)],
        out_specs=[pl.BlockSpec(memory_space=pltpu.VMEM)] * q,
        scratch_shapes=[pltpu.SemaphoreType.DMA] * q,
        compiler_params=pltpu.CompilerParams(vmem_limit_bytes=8 * 2**20),
    )(pltpu.with_memory_space_constraint(texts, pltpu.HBM))
    got = [text_parts[0]]
    for s in range(1, q):
        got.append(shift(text_parts[s], "mp", s))
    image_parts = [images]
    for s in range(1, q):
        image_parts.append(shift(images, "mp", s))
    other_parts = []
    for s in range(q):
        other_parts.append(shift(image_parts[s], "dp", 1))
    text_unit = local_kernel(unit_body, jax.ShapeDtypeStruct((quarter, q * width), BF16), got)
    blocks = [text_unit]
    for d in range(2, n, 2):
        blocks.append(shift(text_unit, "dp", d))
    full = jax.ShapeDtypeStruct((rows, q * width), BF16)
    image_unit = local_kernel(unit_body, full, image_parts)
    other_unit = local_kernel(unit_body, full, other_parts)
    operands = [image_unit, other_unit, *blocks]
    message = pl.pallas_call(
        functools.partial(stats_body, n, q),
        out_shape=jax.ShapeDtypeStruct((n * q, 4, LANES), F32),
        in_specs=[pl.BlockSpec(memory_space=pltpu.SMEM)]
        + [pl.BlockSpec(memory_space=pltpu.VMEM)] * len(operands),
        out_specs=pl.BlockSpec(memory_space=pltpu.VMEM),
        compiler_params=pltpu.CompilerParams(vmem_limit_bytes=8 * 2**20),
    )(logit_scale, *operands)
    answer = lax.all_to_all(message, AXES, 0, 0, tiled=True)
    loss = jax.ShapeDtypeStruct((rows,), F32)
    row_loss, column_loss = local_kernel(
        functools.partial(finish_body, n, q, rows), [loss, loss], [answer]
    )
    return row_loss, column_loss


def gathered(images, texts, logit_scale):
    n = lax.axis_size("dp")
    q = lax.axis_size("mp")
    i = lax.axis_index("dp")
    k = lax.axis_index("mp")
    scale = logit_scale[0]
    rows = images.shape[0]
    quarter = rows // q
    image_unit = normalize(lax.all_gather(images, "mp", axis=1, tiled=True))
    text_unit = normalize(lax.all_to_all(texts, "mp", split_axis=0, concat_axis=1, tiled=True))
    all_texts = lax.all_gather(text_unit, "dp", axis=0, tiled=True)
    scores = scale * lax.dot_general(
        image_unit, all_texts, (((1,), (1,)), ((), ())), preferred_element_type=F32
    )
    row_top = jnp.max(scores, axis=1)
    row_lse = row_top + jnp.log(jnp.sum(jnp.exp(scores - row_top[:, None]), axis=1))
    col_top = jnp.max(scores, axis=0)
    col_lse = col_top + jnp.log(jnp.sum(jnp.exp(scores - col_top[None, :]), axis=0))
    mine = lax.dynamic_slice_in_dim(image_unit, k * quarter, quarter, 0)
    matched = scale * jnp.sum(mine.astype(F32) * text_unit.astype(F32), axis=1)
    pieces = [
        jnp.broadcast_to(row_lse[None], (n, rows)),
        jnp.broadcast_to(matched[None], (n, quarter)),
        col_lse.reshape(n, quarter),
    ]
    message = jnp.concatenate(pieces, axis=1)
    size = message.shape[1]
    lanes = -(-size // LANES) * LANES
    message = jnp.pad(message, ((0, 0), (0, lanes - size)))
    message = jnp.broadcast_to(message[:, None, :], (n, q, lanes)).reshape(n * q, -1, LANES)
    got = lax.all_to_all(message, AXES, 0, 0, tiled=True).reshape(n, q, lanes)
    own = lax.dynamic_index_in_dim(got, i, 0, False)
    row_parts = own[:, :rows]
    peak = jnp.max(row_parts, axis=0)
    row_out = peak + jnp.log(jnp.sum(jnp.exp(row_parts - peak), axis=0))
    matched = own[:, rows : rows + quarter].reshape(rows)
    col_parts = got[:, :, rows + quarter : size]
    peak = jnp.max(col_parts, axis=0)
    col_out = (peak + jnp.log(jnp.sum(jnp.exp(col_parts - peak), axis=0))).reshape(rows)
    return row_out - matched, col_out - matched


def on_device(images, texts, logit_scale):
    n = lax.axis_size("dp")
    q = lax.axis_size("mp")
    power = n & (n - 1) == 0 and q & (q - 1) == 0
    rows, width = images.shape
    fits = LANES < rows <= 2 * LANES and rows // q <= LANES and width % LANES == 0
    if power and n <= 8 and q <= 4 and fits and (rows // q) % 16 == 0:
        return cube(images, texts, logit_scale)
    return gathered(images, texts, logit_scale)


def solution(mesh):
    return jax.shard_map(
        on_device,
        mesh=mesh,
        in_specs=(P("dp", "mp"), P("dp", "mp"), P()),
        out_specs=(P("dp"), P("dp")),
        check_vma=False,
    )
```

```python
import functools

import jax
import jax.numpy as jnp
from jax import lax
from jax.experimental import pallas as pl
from jax.experimental.pallas import tpu as pltpu
from jax.sharding import PartitionSpec as P


AXES = ("dp", "mp")
LANES = 128
F32 = jnp.float32
BF16 = jnp.bfloat16
COST = 50_000_000


def normalize(rows):
    values = rows.astype(F32)
    return (values * lax.rsqrt(jnp.sum(values * values, axis=1, keepdims=True) + 1e-06)).astype(
        BF16
    )


def shift(x, axis, step):
    return lax.ppermute(x, axis, [(i, i ^ step) for i in range(lax.axis_size(axis))])


def local_kernel(body, out_shape, operands, out_memory=pltpu.VMEM):
    outs = jax.tree.leaves(out_shape)
    return pl.pallas_call(
        body,
        out_shape=out_shape,
        in_specs=[pl.BlockSpec(memory_space=pltpu.VMEM)] * len(operands),
        out_specs=jax.tree.map(lambda _: pl.BlockSpec(memory_space=out_memory), out_shape),
        compiler_params=pltpu.CompilerParams(vmem_limit_bytes=8 * 2**20),
    )(*operands)


def split_body(quarter, texts_ref, *out_refs):
    k = lax.axis_index("mp")
    for s, out_ref in enumerate(out_refs):
        start = pl.multiple_of((k ^ s) * quarter, 8)
        out_ref[...] = texts_ref[pl.ds(start, quarter), :]


def unit_body(*refs):
    out_ref = refs[-1]
    parts = [ref[...].astype(F32) for ref in refs[:-1]]
    total = sum(jnp.sum(part * part, axis=1, keepdims=True) for part in parts)
    inverse = lax.rsqrt(total + 1e-06)
    width = parts[0].shape[1]
    for s, part in enumerate(parts):
        out_ref[:, s * width : (s + 1) * width] = (part * inverse).astype(BF16)


def fetch_unit_body(images_ref, *refs):
    part_refs, (own_ref, sem) = refs[:-2], refs[-2:]
    copy = pltpu.make_async_copy(images_ref, own_ref, sem)
    copy.start()
    copy.wait()
    unit_body(own_ref, *part_refs)


def diagonal_body(out_ref):
    row = lax.broadcasted_iota(jnp.int32, out_ref.shape, 0)
    lane = lax.broadcasted_iota(jnp.int32, out_ref.shape, 1)
    out_ref[...] = jnp.where(row == lane, 1.0, 0.0)


def to_lanes(column, diagonal):
    return jnp.sum(jnp.where(diagonal > 0.5, column, 0.0), axis=0, keepdims=True)


def stats_body(n, q, scale_ref, *refs):
    diagonal = refs[0][...]
    image_refs, text_refs, out_ref = refs[1:3], refs[3:-1], refs[-1]
    i = lax.axis_index("dp")
    k = lax.axis_index("mp")
    rows = image_refs[0].shape[0]
    quarter = text_refs[0].shape[0]
    text = jnp.concatenate([ref[...] for ref in text_refs], axis=0)
    scores = [
        scale_ref[...]
        * lax.dot_general(
            text, ref[...], (((1,), (1,)), ((), ())), preferred_element_type=F32
        )
        for ref in image_refs
    ]
    row_lse = []
    for part in scores:
        top = jnp.max(part, axis=0, keepdims=True)
        row_lse.append(top + jnp.log(jnp.sum(jnp.exp(part - top), axis=0, keepdims=True)))
    top = jnp.max(jnp.maximum(*scores), axis=1, keepdims=True)
    total = jnp.exp(scores[0] - top) + jnp.exp(scores[1] - top)
    col_lse = top + jnp.log(jnp.sum(total, axis=1, keepdims=True))
    own = scores[0][:quarter]
    row = lax.broadcasted_iota(jnp.int32, own.shape, 0)
    lane = lax.broadcasted_iota(jnp.int32, own.shape, 1)
    matched = jnp.sum(jnp.where(row + k * quarter == lane, own, 0.0), axis=1, keepdims=True)
    matched = to_lanes(matched, diagonal)
    spare = jnp.zeros((1, 2 * LANES - rows), F32)
    wide = [jnp.concatenate([lse, spare], axis=1) for lse in row_lse]
    for d in range(n):
        lse = wide[d % 2]
        col = to_lanes(col_lse[d // 2 * quarter : (d // 2 + 1) * quarter], diagonal)
        block = jnp.concatenate([lse[:, :LANES], lse[:, LANES:], col, matched], axis=0)
        for m in range(q):
            out_ref[(i ^ d) * q + m] = block


def finish_body(n, q, rows, got_ref, row_ref, col_ref):
    i = lax.axis_index("dp")
    quarter = rows // q

    def merge(parts):
        peak = functools.reduce(jnp.maximum, parts)
        return peak + jnp.log(sum(jnp.exp(x - peak) for x in parts))

    lse = merge([got_ref[(i ^ d) * q + m] for d in range(2) for m in range(q)])
    row_lse = jnp.concatenate([lse[0:1], lse[1:2]], axis=1)[:, :rows]
    own = [got_ref[i * q + m] for m in range(q)]
    matched = jnp.concatenate([x[3:4, :quarter] for x in own], axis=1)
    cols = []
    for m in range(q):
        lse = merge([got_ref[(i ^ d) * q + m] for d in range(0, n, 2)])
        cols.append(lse[2:3, :quarter])
    row_ref[...] = (row_lse - matched).reshape(rows)
    col_ref[...] = (jnp.concatenate(cols, axis=1) - matched).reshape(rows)


def cube(images, texts, logit_scale):
    n = lax.axis_size("dp")
    q = lax.axis_size("mp")
    rows, width = images.shape
    quarter = rows // q
    diagonal = pl.pallas_call(
        diagonal_body,
        out_shape=jax.ShapeDtypeStruct((quarter, LANES), F32),
        out_specs=pl.BlockSpec(memory_space=pltpu.VMEM),
        cost_estimate=pl.CostEstimate(flops=COST, transcendentals=0, bytes_accessed=0),
        compiler_params=pltpu.CompilerParams(vmem_limit_bytes=8 * 2**20),
    )()
    part = jax.ShapeDtypeStruct((quarter, width), BF16)
    text_parts = local_kernel(functools.partial(split_body, quarter), [part] * q, [texts])
    got = [text_parts[0]]
    for s in range(1, q):
        got.append(shift(text_parts[s], "mp", s))
    image_parts = [images]
    for s in range(1, q):
        image_parts.append(shift(images, "mp", s))
    other_parts = []
    for s in range(q):
        other_parts.append(shift(image_parts[s], "dp", 1))
    text_unit = local_kernel(unit_body, jax.ShapeDtypeStruct((quarter, q * width), BF16), got)
    blocks = [text_unit]
    for d in range(2, n, 2):
        blocks.append(shift(text_unit, "dp", d))
    full = jax.ShapeDtypeStruct((rows, q * width), BF16)
    image_unit = pl.pallas_call(
        fetch_unit_body,
        out_shape=full,
        in_specs=[pl.BlockSpec(memory_space=pl.ANY)]
        + [pl.BlockSpec(memory_space=pltpu.VMEM)] * (q - 1),
        out_specs=pl.BlockSpec(memory_space=pltpu.VMEM),
        scratch_shapes=[pltpu.VMEM((rows, width), BF16), pltpu.SemaphoreType.DMA],
        compiler_params=pltpu.CompilerParams(vmem_limit_bytes=8 * 2**20),
    )(pltpu.with_memory_space_constraint(images, pltpu.HBM), *image_parts[1:])
    other_unit = local_kernel(unit_body, full, other_parts)
    operands = [diagonal, image_unit, other_unit, *blocks]
    message = pl.pallas_call(
        functools.partial(stats_body, n, q),
        out_shape=jax.ShapeDtypeStruct((n * q, 4, LANES), F32),
        in_specs=[pl.BlockSpec(memory_space=pltpu.VMEM)] * (len(operands) + 1),
        out_specs=pl.BlockSpec(memory_space=pltpu.VMEM),
        compiler_params=pltpu.CompilerParams(vmem_limit_bytes=8 * 2**20),
    )(logit_scale.reshape(1, 1), *operands)
    answer = lax.all_to_all(message, AXES, 0, 0, tiled=True)
    loss = jax.ShapeDtypeStruct((rows,), F32)
    row_loss, column_loss = local_kernel(
        functools.partial(finish_body, n, q, rows), [loss, loss], [answer]
    )
    return row_loss, column_loss


def gathered(images, texts, logit_scale):
    n = lax.axis_size("dp")
    q = lax.axis_size("mp")
    i = lax.axis_index("dp")
    k = lax.axis_index("mp")
    scale = logit_scale[0]
    rows = images.shape[0]
    quarter = rows // q
    image_unit = normalize(lax.all_gather(images, "mp", axis=1, tiled=True))
    text_unit = normalize(lax.all_to_all(texts, "mp", split_axis=0, concat_axis=1, tiled=True))
    all_texts = lax.all_gather(text_unit, "dp", axis=0, tiled=True)
    scores = scale * lax.dot_general(
        image_unit, all_texts, (((1,), (1,)), ((), ())), preferred_element_type=F32
    )
    row_top = jnp.max(scores, axis=1)
    row_lse = row_top + jnp.log(jnp.sum(jnp.exp(scores - row_top[:, None]), axis=1))
    col_top = jnp.max(scores, axis=0)
    col_lse = col_top + jnp.log(jnp.sum(jnp.exp(scores - col_top[None, :]), axis=0))
    mine = lax.dynamic_slice_in_dim(image_unit, k * quarter, quarter, 0)
    matched = scale * jnp.sum(mine.astype(F32) * text_unit.astype(F32), axis=1)
    pieces = [
        jnp.broadcast_to(row_lse[None], (n, rows)),
        jnp.broadcast_to(matched[None], (n, quarter)),
        col_lse.reshape(n, quarter),
    ]
    message = jnp.concatenate(pieces, axis=1)
    size = message.shape[1]
    lanes = -(-size // LANES) * LANES
    message = jnp.pad(message, ((0, 0), (0, lanes - size)))
    message = jnp.broadcast_to(message[:, None, :], (n, q, lanes)).reshape(n * q, -1, LANES)
    got = lax.all_to_all(message, AXES, 0, 0, tiled=True).reshape(n, q, lanes)
    own = lax.dynamic_index_in_dim(got, i, 0, False)
    row_parts = own[:, :rows]
    peak = jnp.max(row_parts, axis=0)
    row_out = peak + jnp.log(jnp.sum(jnp.exp(row_parts - peak), axis=0))
    matched = own[:, rows : rows + quarter].reshape(rows)
    col_parts = got[:, :, rows + quarter : size]
    peak = jnp.max(col_parts, axis=0)
    col_out = (peak + jnp.log(jnp.sum(jnp.exp(col_parts - peak), axis=0))).reshape(rows)
    return row_out - matched, col_out - matched


def on_device(images, texts, logit_scale):
    n = lax.axis_size("dp")
    q = lax.axis_size("mp")
    power = n & (n - 1) == 0 and q & (q - 1) == 0
    rows, width = images.shape
    fits = LANES < rows <= 2 * LANES and rows // q <= LANES and width % LANES == 0
    if power and n <= 8 and q <= 4 and fits and (rows // q) % 16 == 0:
        return cube(images, texts, logit_scale)
    return gathered(images, texts, logit_scale)


def solution(mesh):
    return jax.shard_map(
        on_device,
        mesh=mesh,
        in_specs=(P("dp", "mp"), P("dp", "mp"), P()),
        out_specs=(P("dp"), P("dp")),
        check_vma=False,
    )
```
